32 devices in a mesh: bank: 4 (over z), zero: 8 (over y, x, core).
Axes of the slice: x: 2, y: 2, z: 4, core: 2. Of those that a mesh axis runs over, the one named last changes fastest.
Arguments:
- master_gate: float32 [64, 2048, 1024], P('bank', 'zero'), may hold values from -0.1875 to 0.1875
- second_gate: bfloat16 [64, 2048, 1024], P('bank', 'zero'), may hold values from -0.0625 to 0.0625
- master_up: float32 [64, 2048, 1024], P('bank', 'zero'), may hold values from -0.1875 to 0.1875
- second_up: bfloat16 [64, 2048, 1024], P('bank', 'zero'), may hold values from -0.0625 to 0.0625
- master_down: float32 [64, 1024, 2048], P('bank', None, 'zero'), may hold values from -0.25 to 0.25
- second_down: bfloat16 [64, 1024, 2048], P('bank', None, 'zero'), may hold values from -0.09375 to 0.09375
- router_weight: float32 [2048, 64], P('zero', 'bank'), may hold values from -0.125 to 0.125
- router_gain: float32 [2048], P('zero'), may hold values from 0.25 to 1.75
Outputs:
- final_gate: bfloat16 [64, 2048, 1024], P('bank', None, 'zero')
- final_up: bfloat16 [64, 2048, 1024], P('bank', None, 'zero')
- final_down: bfloat16 [64, 1024, 2048], P('bank', 'zero')
- scale_gate: float32 [64, 1024], P('bank', 'zero')
- scale_up: float32 [64, 1024], P('bank', 'zero')
- scale_down: float32 [64, 1024], P('bank', 'zero')
- serve_router: bfloat16 [2048, 64], replicated
The draws below stay inside these ranges and needn't reach their ends.
All inputs are finite; a program needn't handle non-finite values. Where the reference program divides by a largest or mean magnitude, that divisor is 1e-20 or more.
Results may differ from the reference program's by a relative error of at most 0.001.
Values may be sent and summed in bfloat16 or wider, within the bound.
A program may use at most 192 MiB of HBM per device.

```python
import jax
import jax.numpy as jnp

EXPERTS = 64
D_MODEL = 2048
D_EXPERT = 1024


def strengthened(array, own_key, source, target, blocks, factor):
    def block_of(dim):
        return (jnp.arange(array.shape[dim]) // (array.shape[dim] // blocks)).reshape((-1,) + (1,) * (array.ndim - 1 - dim))

    one_side = jax.random.permutation(own_key, blocks)[block_of(target)]
    other_side = (block_of(target) + blocks // 2) % blocks
    return jnp.where((block_of(source) == one_side) | (block_of(source) == other_side), factor * array, array)


def levels(rng, extent, cuts, smallest, largest):
    def one(dim, parts):
        heights = jax.random.uniform(jax.random.fold_in(jax.random.fold_in(rng, 6), dim), (parts,), jnp.float32, smallest / len(cuts), largest / len(cuts))
        return jnp.repeat(jnp.exp(heights), extent[dim] // parts).reshape((-1,) + (1,) * (len(extent) - dim - 1))

    factor_of = one(*cuts[0])
    for cut in cuts[1:]:
        factor_of = factor_of * one(*cut)
    return factor_of


def gaussian(key, extent, scale, limit, shards=(), dtype=jnp.bfloat16):
    values = scale * jax.random.normal(key, extent, jnp.float32)
    if shards:
        values = values * levels(key, extent, shards, -0.22, 0.18)
    return jnp.clip(values, -limit, limit).astype(dtype)


def bell_draw_with(stream_key, dims, width, reach, cuts, heavy, dtype=jnp.bfloat16):
    drawn = width * jax.random.normal(stream_key, dims, jnp.float32)
    if cuts:
        drawn = drawn * levels(stream_key, dims, cuts, -0.22, 0.18)
    return jnp.clip(strengthened(drawn, jax.random.fold_in(stream_key, 3), *heavy), -reach, reach).astype(dtype)


def setup_inputs(seed: int = 0) -> dict:
    keys = jax.random.split(jax.random.key(seed), 9)
    return {
        "master_gate": bell_draw_with(keys[0], (EXPERTS, D_MODEL, D_EXPERT), D_MODEL ** -0.5, 0.1875, ((0, 4), (1, 8)), (1, 2, 8, 2.0), jnp.float32),
        "second_gate": gaussian(keys[1], (EXPERTS, D_MODEL, D_EXPERT), (D_MODEL * 4) ** -0.5, 0.0625, ((0, 4), (1, 8))),
        "master_up": bell_draw_with(keys[2], (EXPERTS, D_MODEL, D_EXPERT), D_MODEL ** -0.5, 0.1875, ((0, 4), (1, 8)), (1, 2, 8, 2.0), jnp.float32),
        "second_up": gaussian(keys[3], (EXPERTS, D_MODEL, D_EXPERT), (D_MODEL * 4) ** -0.5, 0.0625, ((0, 4), (1, 8))),
        "master_down": bell_draw_with(keys[4], (EXPERTS, D_EXPERT, D_MODEL), D_EXPERT ** -0.5, 0.25, ((0, 4), (2, 8)), (2, 1, 8, 2.0), jnp.float32),
        "second_down": gaussian(keys[5], (EXPERTS, D_EXPERT, D_MODEL), (D_EXPERT * 4) ** -0.5, 0.09375, ((0, 4), (2, 8))),
        "router_weight": gaussian(keys[6], (D_MODEL, EXPERTS), D_MODEL ** -0.5, 0.125, ((0, 8), (1, 4)), jnp.float32),
        "router_gain": jnp.clip(1.0 + 0.15 * jax.random.normal(keys[7], (D_MODEL,), jnp.float32), 0.25, 1.75),
    }


def reference(master_gate, second_gate, master_up, second_up, master_down, second_down, router_weight, router_gain):
    merged_gate = master_gate + second_gate.astype(jnp.float32)
    merged_up = master_up + second_up.astype(jnp.float32)
    merged_down = master_down + second_down.astype(jnp.float32)
    scale_gate = jnp.sum(jnp.abs(merged_gate), axis=1) / D_MODEL
    final_gate = (merged_gate / jnp.expand_dims(scale_gate, 1)).astype(jnp.bfloat16)
    scale_up = jnp.sum(jnp.abs(merged_up), axis=1) / D_MODEL
    final_up = (merged_up / jnp.expand_dims(scale_up, 1)).astype(jnp.bfloat16)
    scale_down = jnp.sum(jnp.abs(merged_down), axis=2) / D_MODEL
    final_down = (merged_down / jnp.expand_dims(scale_down, 2)).astype(jnp.bfloat16)
    serve_router = (router_weight * router_gain[:, None]).astype(jnp.bfloat16)
    return final_gate, final_up, final_down, scale_gate, scale_up, scale_down, serve_router
```

```python
import functools

import jax
import jax.numpy as jnp
from jax import lax
from jax.experimental import pallas as pl
from jax.experimental.pallas import tpu as pltpu
from jax.sharding import PartitionSpec as P

f32, bf16 = jnp.float32, jnp.bfloat16
MESH = pl.DeviceIdType.MESH
GROUP = 8
FIRST = 2
AHEAD = 4
READS = 2
SLOTS = 4


def flip(index, bits, size):
    out, bit = 0, 1
    while bit < size:
        own = (index // bit) % 2
        out = out + bit * ((1 - own) if bits & bit else own)
        bit *= 2
    return out


def send_order(zero):
    return sorted(range(1, zero), key=lambda d: (d == 1, d & 1, -d))


def exchange_kernel(bank, zero, *refs):
    (mg, sg, mu, su, md, sd, rw, gain,
     land_gate, land_up, land_down, scale_gate, scale_up, scale_down, router,
     sum_m, sum_s, sum_dm, sum_ds, in_m, in_s, in_dm, in_ds, stage, stage_down,
     first, first_got, first_inv, part, part_got, total, inverse,
     rw_v, gain_v, router_part,
     sum_sem, in_sem, stage_sem, data_sem, small_sem, router_sem) = refs
    experts, rows, width = mg.shape
    piece = width // zero
    model = rows * zero
    per = experts // GROUP
    me = lax.axis_index("zero")
    my_bank = lax.axis_index("bank")
    masters, seconds = (mg, mu, md), (sg, su, sd)
    lands = (land_gate, land_up, land_down)
    scales = (scale_gate, scale_up, scale_down)
    order = send_order(zero)

    def peer(d):
        return flip(me, d, zero)

    def columns(k):
        return pl.ds(pl.multiple_of(k * piece, piece), piece)

    def send(src, dst, send_sem, recv_sem, d):
        pltpu.make_async_remote_copy(
            src_ref=src, dst_ref=dst, send_sem=send_sem, recv_sem=recv_sem,
            device_id={"zero": peer(d)}, device_id_type=MESH,
        ).start()

    def await_bytes(ref, sem):
        pltpu.make_async_copy(ref, ref, sem).wait()

    def reads(m, e, slot, bufs, sem):
        return (
            pltpu.make_async_copy(masters[m].at[e], bufs[0].at[slot], sem.at[0, slot]),
            pltpu.make_async_copy(seconds[m].at[e], bufs[1].at[slot], sem.at[1, slot]),
        )

    def sum_reads(m, e, slot):
        bufs = (sum_m, sum_s) if m < 2 else (sum_dm, sum_ds)
        return reads(m, e, slot, bufs, sum_sem.at[int(m == 2)])

    def scale_reads(m, e, slot):
        bufs = (in_m, in_s) if m < 2 else (in_dm, in_ds)
        return reads(m, e, slot, bufs, in_sem.at[int(m == 2)])

    def start(copies):
        for c in copies:
            c.start()

    def finish(copies):
        for c in copies:
            c.wait()


    def row_sum(m_ref, s_ref):
        def body(i, acc):
            r = pl.ds(pl.multiple_of(i * 16, 16), 16)
            x = jnp.abs(m_ref[r, :] + s_ref[r, :].astype(f32))
            return acc + (x[:8] + x[8:])

        acc = lax.fori_loop(0, rows // 16, body, jnp.zeros((8, width), f32), unroll=4)
        return jnp.sum(acc, axis=0, keepdims=True)

    def store_column_sums(m_ref, s_ref, g, j):
        found = []
        for k in range(width // 128):
            r = slice(k * 128, (k + 1) * 128)
            acc = None
            for c in range(rows // 128):
                cut = slice(c * 128, (c + 1) * 128)
                x = jnp.abs(m_ref[r, cut] + s_ref[r, cut].astype(f32))
                acc = x if acc is None else acc + x
            found.append(jnp.sum(acc.T, axis=0, keepdims=True))
        part[g, pl.ds(j, 1), :] = jnp.concatenate(found, axis=1)

    def sum_experts(g, low, high, last=True):
        m, base = g // per, (g % per) * GROUP

        def body(j, _):
            slot = lax.rem(j, AHEAD)
            finish(sum_reads(m, base + j, slot))
            if m < 2:
                v = row_sum(sum_m.at[slot], sum_s.at[slot])
                part[g, pl.ds(j, 1), :] = v
                if high == FIRST:
                    first[pl.ds(j, 1), :] = v
            else:
                store_column_sums(sum_dm.at[slot], sum_ds.at[slot], g, j)

            @pl.when(j + AHEAD < GROUP)
            def _():
                start(sum_reads(m, base + j + AHEAD, slot))

            return 0

        lax.fori_loop(low, high, body, 0)
        if last and g + 1 < 3 * per:
            for j in range(AHEAD):
                start(sum_reads((g + 1) // per, ((g + 1) % per) * GROUP + j, j))

    def scatter_sums(g):
        for d in order:
            send(part.at[g, :, columns(peer(d))], part_got.at[g, d - 1],
                 small_sem.at[0, g], small_sem.at[1, g], d)

    def gather_totals(g):
        await_bytes(part_got.at[g], small_sem.at[1, g])
        t = part[g, :, columns(me)]
        for d in range(1, zero):
            t = t + part_got[g, d - 1]
        total[g, :, columns(me)] = t
        m, base = g // per, (g % per) * GROUP
        scales[m][base : base + GROUP, :] = t / model
        for d in order:
            mine = total.at[g, :, columns(me)]
            send(mine, mine, small_sem.at[2, g], small_sem.at[3, g], d)

    def take_totals(g):
        await_bytes(part_got.at[g], small_sem.at[3, g])
        for k in range(zero):
            inverse[g, k] = 1.0 / (total[g, :, k * piece : (k + 1) * piece] / model)


    def send_expert(m, e, row, slot, fresh=False):
        finish(scale_reads(m, e, lax.rem(e, READS)))
        b = lax.rem(e, READS)
        staged = stage if m < 2 else stage_down
        sem = stage_sem.at[int(m == 2), slot]
        if not fresh:
            await_bytes(staged.at[slot], sem)
        half = rows // 2
        for d in order + [0]:
            k = peer(d)
            cut = columns(k)
            scale = row(k)
            if m < 2:
                for h in range(2):
                    r = slice(h * half, (h + 1) * half)
                    x = (in_m[b, r, cut] + in_s[b, r, cut].astype(f32)) * scale
                    if d:
                        stage[slot, d - 1, r, :] = x.astype(bf16)
                    else:
                        at = pl.ds(pl.multiple_of(me * rows + h * half, half), half)
                        lands[m][e, at, :] = x.astype(bf16)
                there = lands[m].at[e, pl.ds(pl.multiple_of(me * rows, rows), rows)]
            else:
                t = jnp.broadcast_to(scale, (128, piece)).T
                for c in range(rows // 128):
                    r = slice(c * 128, (c + 1) * 128)
                    x = (in_dm[b, cut, r] + in_ds[b, cut, r].astype(f32)) * t
                    if d:
                        stage_down[slot, d - 1, :, r] = x.astype(bf16)
                    else:
                        land_down[e, me, :, r] = x.astype(bf16)
                there = land_down.at[e, me]
            if d:
                send(staged.at[slot, d - 1], there, sem, data_sem.at[m, d - 1], d)

    def scaled_row(g, j):
        return lambda k: inverse[g, k, pl.ds(j, 1), :]

    def send_range(m, low, high, fresh=False):
        def body(e, _):
            send_expert(m, e, scaled_row(m * per + e // GROUP, lax.rem(e, GROUP)),
                        lax.rem(e, SLOTS), fresh)

            @pl.when(e + READS < experts)
            def _():
                start(scale_reads(m, e + READS, lax.rem(e, READS)))

            return 0

        lax.fori_loop(low, high, body, 0)


    c = rw.shape[0]
    own_experts = pl.ds(pl.multiple_of(my_bank * c, c), c)
    own_rows = pl.ds(pl.multiple_of(me * rows, rows), rows)

    def router_reads():
        return (
            pltpu.make_async_copy(rw, rw_v, router_sem.at[0]),
            pltpu.make_async_copy(gain, gain_v, router_sem.at[1]),
        )

    def send_router():
        finish(router_reads())
        router_part[...] = (rw_v[...] * gain_v[...]).astype(bf16)
        router[own_experts, own_rows] = router_part[...]
        for d in order:
            send(router_part, router.at[own_experts, own_rows], router_sem.at[2], router_sem.at[3], d)

    def share_router():
        await_bytes(router.at[pl.ds(0, c), pl.ds(0, (zero - 1) * rows)], router_sem.at[3])
        for d in range(1, bank):
            pltpu.make_async_remote_copy(
                src_ref=router.at[own_experts], dst_ref=router.at[own_experts],
                send_sem=router_sem.at[4], recv_sem=router_sem.at[5],
                device_id={"bank": (my_bank + d) % bank}, device_id_type=MESH,
            ).start()


    barrier = pltpu.get_barrier_semaphore()
    for d in range(1, zero):
        pl.semaphore_signal(barrier, inc=1, device_id={"zero": peer(d)}, device_id_type=MESH)
    for d in range(1, bank):
        pl.semaphore_signal(
            barrier, inc=1, device_id={"bank": (my_bank + d) % bank}, device_id_type=MESH)

    for j in range(AHEAD):
        start(sum_reads(0, j, j))
    for j in range(READS):
        start(scale_reads(0, j, j))
        start(scale_reads(2, j, j))
    start(router_reads())
    sum_experts(0, 0, FIRST, last=False)
    pl.semaphore_wait(barrier, zero - 1 + bank - 1)
    for d in order:
        send(first, first_got.at[d - 1], small_sem.at[4, 0], small_sem.at[4, 1], d)
    sum_experts(0, FIRST, GROUP)
    scatter_sums(0)
    await_bytes(first_got, small_sem.at[4, 1])
    t = first[...]
    for d in range(1, zero):
        t = t + first_got[d - 1]
    for k in range(zero):
        first_inv[k] = 1.0 / (t[:, k * piece : (k + 1) * piece] / model)

    def send_first(j):
        send_expert(0, j, lambda k: first_inv[k, j : j + 1, :], j, fresh=True)
        start(scale_reads(0, j + READS, j % READS))

    send_first(0)
    sum_experts(1, 0, GROUP)
    scatter_sums(1)
    gather_totals(0)
    send_first(1)
    send_router()
    take_totals(0)
    send_range(0, 2, 4, fresh=True)
    gather_totals(1)
    sum_experts(2, 0, GROUP)
    scatter_sums(2)
    send_range(0, 4, 6)
    sum_experts(3, 0, GROUP)
    scatter_sums(3)
    send_range(0, 6, 7)
    gather_totals(2)
    send_range(0, 7, 8)
    take_totals(1)
    send_range(0, 8, 10)
    sum_experts(4, 0, GROUP)
    scatter_sums(4)
    gather_totals(3)
    send_range(0, 10, 12)
    sum_experts(5, 0, GROUP)
    scatter_sums(5)
    share_router()
    send_range(0, 12, 14)
    gather_totals(4)
    send_range(0, 14, 16)
    for j in range(READS):
        start(scale_reads(1, j, j))
    gather_totals(5)
    take_totals(2)
    take_totals(3)
    send_range(1, 0, 4)
    take_totals(4)
    take_totals(5)
    send_range(1, 4, 16)
    send_range(2, 0, SLOTS, fresh=True)
    send_range(2, SLOTS, experts)

    for s in range(SLOTS):
        await_bytes(stage.at[s], stage_sem.at[0, s])
        await_bytes(stage_down.at[s], stage_sem.at[1, s])
    await_bytes(first_got, small_sem.at[4, 0])
    for g in range(3 * per):
        await_bytes(part_got.at[g], small_sem.at[0, g])
        await_bytes(part_got.at[g], small_sem.at[2, g])
    await_bytes(router.at[pl.ds(0, c), pl.ds(0, (zero - 1) * rows)], router_sem.at[2])
    if bank > 1:
        await_bytes(router.at[pl.ds(0, (bank - 1) * c)], router_sem.at[4])
        await_bytes(router.at[pl.ds(0, (bank - 1) * c)], router_sem.at[5])
    for d in range(1, zero):
        await_bytes(land_gate.at[:, pl.ds(0, rows)], data_sem.at[0, d - 1])
        await_bytes(land_up.at[:, pl.ds(0, rows)], data_sem.at[1, d - 1])
        await_bytes(land_down.at[:, 0], data_sem.at[2, d - 1])


def store_kernel(zero, *refs):
    gate, up, down, *small = refs[:7]
    out_gate, out_up, out_down, *small_out = refs[7:14]
    sem = refs[14]
    rows = down.shape[3]
    copies = []
    for src, dst in ((gate, out_gate), (up, out_up)):
        for k in range(zero):
            at = pl.ds(k * (src.shape[0] // zero), src.shape[0] // zero)
            copies.append((src.at[at], dst.at[at]))
    for k in range(zero):
        copies.append((down.at[:, k], out_down.at[:, :, k * rows : (k + 1) * rows]))
    copies += list(zip(small, small_out))
    copies = [pltpu.make_async_copy(s, d, sem.at[i]) for i, (s, d) in enumerate(copies)]
    for c in copies:
        c.start()
    for c in copies:
        c.wait()


def fast_device(sizes, mg, sg, mu, su, md, sd, router_weight, router_gain):
    bank, zero = sizes
    experts, rows, width = mg.shape
    piece = width // zero
    c = router_weight.shape[1]
    groups = 3 * experts // GROUP
    anywhere = pl.BlockSpec(memory_space=pl.ANY)
    vmem = pl.BlockSpec(memory_space=pltpu.VMEM)
    shapes = (
        ((experts, zero * rows, piece), bf16),
        ((experts, zero * rows, piece), bf16),
        ((experts, zero, piece, rows), bf16),
        ((experts, piece), f32),
        ((experts, piece), f32),
        ((experts, piece), f32),
        ((bank * c, zero * rows), bf16),
    )
    dma = pltpu.SemaphoreType.DMA
    landed = pl.pallas_call(
        functools.partial(exchange_kernel, bank, zero),
        in_specs=[anywhere] * 8,
        out_specs=[vmem] * 7,
        out_shape=[pltpu.VMEM(*s) for s in shapes],
        scratch_shapes=[
            pltpu.VMEM((AHEAD, rows, width), f32),
            pltpu.VMEM((AHEAD, rows, width), bf16),
            pltpu.VMEM((AHEAD, width, rows), f32),
            pltpu.VMEM((AHEAD, width, rows), bf16),
            pltpu.VMEM((READS, rows, width), f32),
            pltpu.VMEM((READS, rows, width), bf16),
            pltpu.VMEM((READS, width, rows), f32),
            pltpu.VMEM((READS, width, rows), bf16),
            pltpu.VMEM((SLOTS, zero - 1, rows, piece), bf16),
            pltpu.VMEM((SLOTS, zero - 1, piece, rows), bf16),
            pltpu.VMEM((FIRST, width), f32),
            pltpu.VMEM((zero - 1, FIRST, width), f32),
            pltpu.VMEM((zero, FIRST, piece), f32),
            pltpu.VMEM((groups, GROUP, width), f32),
            pltpu.VMEM((groups, zero - 1, GROUP, piece), f32),
            pltpu.VMEM((groups, GROUP, width), f32),
            pltpu.VMEM((groups, zero, GROUP, piece), f32),
            pltpu.VMEM((c, rows), f32),
            pltpu.VMEM((1, rows), f32),
            pltpu.VMEM((c, rows), bf16),
            dma((2, 2, AHEAD)),
            dma((2, 2, READS)),
            dma((2, SLOTS)),
            dma((3, zero - 1)),
            dma((5, groups)),
            dma((6,)),
        ],
        compiler_params=pltpu.CompilerParams(
            collective_id=0, has_side_effects=True, vmem_limit_bytes=34 << 20),
    )(mg, sg, mu, su, md, sd, router_weight.T, router_gain.reshape(1, -1))
    outs = shapes[:2] + (((experts, piece, zero * rows), bf16),) + shapes[3:]
    *stored, router = pl.pallas_call(
        functools.partial(store_kernel, zero),
        in_specs=[vmem] * 7,
        out_specs=[anywhere] * 7,
        out_shape=[jax.ShapeDtypeStruct(*s) for s in outs],
        scratch_shapes=[dma((3 * zero + 4,))],
        compiler_params=pltpu.CompilerParams(vmem_limit_bytes=1 << 20),
    )(*landed)
    return (*stored, router.T)


def mine(scale, zero):
    width = scale.shape[1] // zero
    return lax.dynamic_slice_in_dim(scale, lax.axis_index("zero") * width, width, axis=1)


def general_device(sizes, mg, sg, mu, su, md, sd, router_weight, router_gain):
    zero = sizes[1]
    model = mg.shape[1] * zero
    merged = (mg + sg.astype(f32), mu + su.astype(f32), md + sd.astype(f32))
    totals = lax.psum(
        tuple(jnp.sum(jnp.abs(m), axis=a) for m, a in zip(merged, (1, 1, 2))), "zero"
    )
    scales = tuple(t / model for t in totals)
    finals = tuple(
        lax.all_to_all(
            (m / jnp.expand_dims(s, a)).astype(bf16),
            "zero", split_axis=3 - a, concat_axis=a, tiled=True,
        )
        for m, s, a in zip(merged, scales, (1, 1, 2))
    )
    part_router = (router_weight * router_gain[:, None]).astype(bf16)
    row_router = lax.all_gather(part_router, "zero", axis=0, tiled=True)
    serve_router = lax.all_gather(row_router, "bank", axis=1, tiled=True)
    return finals + tuple(mine(s, zero) for s in scales) + (serve_router,)


def fits(sizes, mg, router_weight):
    zero = sizes[1]
    experts, rows, width = mg.shape
    c = router_weight.shape[1]
    if zero < 2 or zero & (zero - 1) or experts != 2 * GROUP or experts % zero:
        return False
    if width % zero or (width // zero) % 128 or rows % 256 or c % 16:
        return False
    unit = rows * width
    held = 3 * experts * unit * 2 + 2 * (6 * (AHEAD + READS) + 2 * SLOTS) * unit
    return held <= 52 << 20


def solution(mesh):
    sizes = (mesh.shape["bank"], mesh.shape["zero"])

    def on_device(*args):
        fast = fits(sizes, args[0], args[6])
        return (fast_device if fast else general_device)(sizes, *args)

    return jax.shard_map(
        on_device,
        mesh=mesh,
        in_specs=(
            P("bank", "zero", None),
            P("bank", "zero", None),
            P("bank", "zero", None),
            P("bank", "zero", None),
            P("bank", None, "zero"),
            P("bank", None, "zero"),
            P("zero", "bank"),
            P("zero"),
        ),
        out_specs=(
            P("bank", None, "zero"),
            P("bank", None, "zero"),
            P("bank", "zero", None),
            P("bank", "zero"),
            P("bank", "zero"),
            P("bank", "zero"),
            P(),
        ),
        check_vma=False,
    )
```

```python
import functools

import jax
import jax.numpy as jnp
from jax import lax
from jax.experimental import pallas as pl
from jax.experimental.pallas import tpu as pltpu
from jax.sharding import PartitionSpec as P

f32, bf16 = jnp.float32, jnp.bfloat16
MESH = pl.DeviceIdType.MESH
GROUP = 8
FIRST = 2
AHEAD = 4
READS = 2
SLOTS = 4


def flip(index, bits, size):
    out, bit = 0, 1
    while bit < size:
        own = (index // bit) % 2
        out = out + bit * ((1 - own) if bits & bit else own)
        bit *= 2
    return out


def send_order(zero):
    return sorted(range(1, zero), key=lambda d: (d == 1, d & 1, -d))


def exchange_kernel(bank, zero, *refs):
    (mg, sg, mu, su, md, sd, rw, gain,
     land_gate, land_up, land_down, scale_gate, scale_up, scale_down, router,
     sum_m, sum_s, sum_dm, sum_ds, in_m, in_s, in_dm, in_ds, stage, stage_down,
     first, first_got, first_inv, part, part_got, pair_got, fold, fold_got, total, inverse,
     rw_v, gain_v, router_part,
     sum_sem, in_sem, stage_sem, data_sem, small_sem, fold_sem, router_sem) = refs
    experts, rows, width = mg.shape
    piece = width // zero
    model = rows * zero
    per = experts // GROUP
    me = lax.axis_index("zero")
    my_bank = lax.axis_index("bank")
    masters, seconds = (mg, mu, md), (sg, su, sd)
    lands = (land_gate, land_up, land_down)
    scales = (scale_gate, scale_up, scale_down)
    order = send_order(zero)
    folds = fold_sem.shape[0] // 2 - 2
    half = width // 2
    my_half = pl.ds(pl.multiple_of((me % 2) * half, half), half)
    its_half = pl.ds(pl.multiple_of((1 - me % 2) * half, half), half)

    def peer(d):
        return flip(me, d, zero)

    def columns(k):
        return pl.ds(pl.multiple_of(k * piece, piece), piece)

    def send(src, dst, send_sem, recv_sem, d):
        pltpu.make_async_remote_copy(
            src_ref=src, dst_ref=dst, send_sem=send_sem, recv_sem=recv_sem,
            device_id={"zero": peer(d)}, device_id_type=MESH,
        ).start()

    def await_bytes(ref, sem):
        pltpu.make_async_copy(ref, ref, sem).wait()

    def reads(m, e, slot, bufs, sem):
        return (
            pltpu.make_async_copy(masters[m].at[e], bufs[0].at[slot], sem.at[0, slot]),
            pltpu.make_async_copy(seconds[m].at[e], bufs[1].at[slot], sem.at[1, slot]),
        )

    def sum_reads(m, e, slot):
        bufs = (sum_m, sum_s) if m < 2 else (sum_dm, sum_ds)
        return reads(m, e, slot, bufs, sum_sem.at[int(m == 2)])

    def scale_reads(m, e, slot):
        bufs = (in_m, in_s) if m < 2 else (in_dm, in_ds)
        return reads(m, e, slot, bufs, in_sem.at[int(m == 2)])

    def start(copies):
        for c in copies:
            c.start()

    def finish(copies):
        for c in copies:
            c.wait()


    def row_sum(m_ref, s_ref):
        def body(i, acc):
            r = pl.ds(pl.multiple_of(i * 16, 16), 16)
            x = jnp.abs(m_ref[r, :] + s_ref[r, :].astype(f32))
            return acc + (x[:8] + x[8:])

        acc = lax.fori_loop(0, rows // 16, body, jnp.zeros((8, width), f32), unroll=4)
        return jnp.sum(acc, axis=0, keepdims=True)

    def store_column_sums(m_ref, s_ref, g, j):
        found = []
        for k in range(width // 128):
            r = slice(k * 128, (k + 1) * 128)
            acc = None
            for c in range(rows // 128):
                cut = slice(c * 128, (c + 1) * 128)
                x = jnp.abs(m_ref[r, cut] + s_ref[r, cut].astype(f32))
                acc = x if acc is None else acc + x
            found.append(jnp.sum(acc.T, axis=0, keepdims=True))
        part[g, pl.ds(j, 1), :] = jnp.concatenate(found, axis=1)

    def sum_first():
        for j in range(FIRST):
            finish(scale_reads(0, j, j))
            v = row_sum(in_m.at[j], in_s.at[j])
            part[0, j : j + 1, :] = v
            first[j : j + 1, :] = v

    def sum_experts(g, low=0):
        m, base = g // per, (g % per) * GROUP

        def body(j, _):
            slot = lax.rem(j, AHEAD)
            finish(sum_reads(m, base + j, slot))
            if m < 2:
                v = row_sum(sum_m.at[slot], sum_s.at[slot])
                part[g, pl.ds(j, 1), :] = v
            else:
                store_column_sums(sum_dm.at[slot], sum_ds.at[slot], g, j)

            @pl.when(j + AHEAD < GROUP)
            def _():
                start(sum_reads(m, base + j + AHEAD, slot))

            return 0

        lax.fori_loop(low, GROUP, body, 0)
        if g + 1 < 3 * per:
            for j in range(AHEAD):
                start(sum_reads((g + 1) // per, ((g + 1) % per) * GROUP + j, j))

    def scatter_sums():
        for d in order:
            send(part.at[0, :, columns(peer(d))], part_got.at[d - 1],
                 small_sem.at[0], small_sem.at[1], d)

    def gather_totals():
        await_bytes(part_got, small_sem.at[1])
        t = part[0, :, columns(me)]
        for d in range(1, zero):
            t = t + part_got[d - 1]
        total[0, :, columns(me)] = t
        scales[0][:GROUP, :] = t / model
        for d in order:
            mine = total.at[0, :, columns(me)]
            send(mine, mine, small_sem.at[2], small_sem.at[3], d)

    def take_totals(g):
        if g:
            await_bytes(pair_got.at[g], fold_sem.at[2 * folds + 3, g])
            m, base = g // per, (g % per) * GROUP
            scales[m][base : base + GROUP, :] = total[g, :, columns(me)] / model
        else:
            await_bytes(part_got, small_sem.at[3])
        for k in range(zero):
            inverse[g, k] = 1.0 / (total[g, :, k * piece : (k + 1) * piece] / model)

    def pair_sums(g):
        send(part.at[g, :, its_half], pair_got.at[g], fold_sem.at[0, g], fold_sem.at[1, g], 1)

    def fold_sums(g, i):
        for i in range(i, folds + 1 if i == 2 else min(i, folds) + 1):
            if i:
                await_bytes(pair_got.at[g], fold_sem.at[2 * i + 1, g])
                h = fold[g, i - 1] + fold_got[g, i - 1]
            else:
                await_bytes(pair_got.at[g], fold_sem.at[1, g])
                h = part[g, :, my_half] + pair_got[g]
            sems = fold_sem.at[2 * i + 2, g], fold_sem.at[2 * i + 3, g]
            if i < folds:
                fold[g, i] = h
                send(fold.at[g, i], fold_got.at[g, i], *sems, 2 << i)
            else:
                total[g, :, my_half] = h
                there = total.at[g, :, my_half]
                send(there, there, *sems, 1)


    def send_expert(m, e, row, slot, fresh=False, ready=False):
        if not ready:
            finish(scale_reads(m, e, lax.rem(e, READS)))
        b = lax.rem(e, READS)
        staged = stage if m < 2 else stage_down
        sem = stage_sem.at[int(m == 2), slot]
        if not fresh:
            await_bytes(staged.at[slot], sem)
        lot = rows // 2
        for d in order + [0]:
            k = peer(d)
            cut = columns(k)
            scale = row(k)
            if m < 2:
                for h in range(2):
                    r = slice(h * lot, (h + 1) * lot)
                    x = (in_m[b, r, cut] + in_s[b, r, cut].astype(f32)) * scale
                    if d:
                        stage[slot, d - 1, r, :] = x.astype(bf16)
                    else:
                        at = pl.ds(pl.multiple_of(me * rows + h * lot, lot), lot)
                        lands[m][e, at, :] = x.astype(bf16)
                there = lands[m].at[e, pl.ds(pl.multiple_of(me * rows, rows), rows)]
            else:
                t = jnp.broadcast_to(scale, (128, piece)).T
                for c in range(rows // 128):
                    r = slice(c * 128, (c + 1) * 128)
                    x = (in_dm[b, cut, r] + in_ds[b, cut, r].astype(f32)) * t
                    if d:
                        stage_down[slot, d - 1, :, r] = x.astype(bf16)
                    else:
                        land_down[e, me, :, r] = x.astype(bf16)
                there = land_down.at[e, me]
            if d:
                send(staged.at[slot, d - 1], there, sem, data_sem.at[m, d - 1], d)

    def scaled_row(g, j):
        return lambda k: inverse[g, k, pl.ds(j, 1), :]

    def send_range(m, low, high, fresh=False):
        def body(e, _):
            send_expert(m, e, scaled_row(m * per + e // GROUP, lax.rem(e, GROUP)),
                        lax.rem(e, SLOTS), fresh)

            @pl.when(e + READS < experts)
            def _():
                start(scale_reads(m, e + READS, lax.rem(e, READS)))

            return 0

        lax.fori_loop(low, high, body, 0)


    c = rw.shape[0]
    own_experts = pl.ds(pl.multiple_of(my_bank * c, c), c)
    own_rows = pl.ds(pl.multiple_of(me * rows, rows), rows)

    def router_reads():
        return (
            pltpu.make_async_copy(rw, rw_v, router_sem.at[0]),
            pltpu.make_async_copy(gain, gain_v, router_sem.at[1]),
        )

    def fold_router():
        finish(router_reads())
        router_part[...] = (rw_v[...] * gain_v[...]).astype(bf16)
        router[own_experts, own_rows] = router_part[...]

    def send_router():
        for d in order:
            send(router_part, router.at[own_experts, own_rows], router_sem.at[2], router_sem.at[3], d)

    def share_router():
        await_bytes(router.at[pl.ds(0, c), pl.ds(0, (zero - 1) * rows)], router_sem.at[3])
        for d in range(1, bank):
            pltpu.make_async_remote_copy(
                src_ref=router.at[own_experts], dst_ref=router.at[own_experts],
                send_sem=router_sem.at[4], recv_sem=router_sem.at[5],
                device_id={"bank": (my_bank + d) % bank}, device_id_type=MESH,
            ).start()


    barrier = pltpu.get_barrier_semaphore()
    for d in range(1, zero):
        pl.semaphore_signal(barrier, inc=1, device_id={"zero": peer(d)}, device_id_type=MESH)
    for d in range(1, bank):
        pl.semaphore_signal(
            barrier, inc=1, device_id={"bank": (my_bank + d) % bank}, device_id_type=MESH)

    start(router_reads())
    for j in range(FIRST):
        start(scale_reads(0, j, j))
    fold_router()
    for j in range(FIRST, FIRST + AHEAD):
        start(sum_reads(0, j, j % AHEAD))
    sum_first()
    pl.semaphore_wait(barrier, zero - 1 + bank - 1)
    for d in order:
        send(first, first_got.at[d - 1], small_sem.at[4], small_sem.at[5], d)
    send_router()
    sum_experts(0, FIRST)
    scatter_sums()
    await_bytes(first_got, small_sem.at[5])
    t = first[...]
    for d in range(1, zero):
        t = t + first_got[d - 1]
    for k in range(zero):
        first_inv[k] = 1.0 / (t[:, k * piece : (k + 1) * piece] / model)

    def send_first(j):
        send_expert(0, j, lambda k: first_inv[k, j : j + 1, :], j, fresh=True, ready=True)
        start(scale_reads(0, j + READS, j % READS))

    send_first(0)
    sum_experts(1)
    pair_sums(1)
    gather_totals()
    send_first(1)
    fold_sums(1, 0)
    take_totals(0)
    send_range(0, 2, 4, fresh=True)
    sum_experts(2)
    pair_sums(2)
    fold_sums(1, 1)
    fold_sums(2, 0)
    send_range(0, 4, 6)
    fold_sums(1, 2)
    fold_sums(2, 1)
    sum_experts(3)
    pair_sums(3)
    send_range(0, 6, 7)
    fold_sums(3, 0)
    send_range(0, 7, 8)
    take_totals(1)
    send_range(0, 8, 10)
    fold_sums(2, 2)
    fold_sums(3, 1)
    sum_experts(4)
    pair_sums(4)
    send_range(0, 10, 11)
    fold_sums(4, 0)
    send_range(0, 11, 12)
    fold_sums(3, 2)
    fold_sums(4, 1)
    sum_experts(5)
    pair_sums(5)
    send_range(0, 12, 13)
    fold_sums(5, 0)
    share_router()
    send_range(0, 13, 14)
    fold_sums(4, 2)
    fold_sums(5, 1)
    send_range(0, 14, 16)
    for j in range(READS):
        start(scale_reads(1, j, j))
        start(scale_reads(2, j, j))
    fold_sums(5, 2)
    take_totals(2)
    take_totals(3)
    send_range(1, 0, 2)
    take_totals(4)
    take_totals(5)
    send_range(1, 2, experts)
    send_range(2, 0, SLOTS, fresh=True)
    send_range(2, SLOTS, experts)

    for s in range(SLOTS):
        await_bytes(stage.at[s], stage_sem.at[0, s])
        await_bytes(stage_down.at[s], stage_sem.at[1, s])
    await_bytes(first_got, small_sem.at[4])
    await_bytes(part_got, small_sem.at[0])
    await_bytes(part_got, small_sem.at[2])
    for g in range(1, 3 * per):
        for i in range(folds + 2):
            await_bytes(pair_got.at[g], fold_sem.at[2 * i, g])
    await_bytes(router.at[pl.ds(0, c), pl.ds(0, (zero - 1) * rows)], router_sem.at[2])
    if bank > 1:
        await_bytes(router.at[pl.ds(0, (bank - 1) * c)], router_sem.at[4])
        await_bytes(router.at[pl.ds(0, (bank - 1) * c)], router_sem.at[5])
    for d in range(1, zero):
        await_bytes(land_gate.at[:, pl.ds(0, rows)], data_sem.at[0, d - 1])
        await_bytes(land_up.at[:, pl.ds(0, rows)], data_sem.at[1, d - 1])
        await_bytes(land_down.at[:, 0], data_sem.at[2, d - 1])


def store_kernel(zero, *refs):
    gate, up, down, *small = refs[:7]
    out_gate, out_up, out_down, *small_out = refs[7:14]
    sem = refs[14]
    rows = down.shape[3]
    copies = []
    for src, dst in ((gate, out_gate), (up, out_up)):
        for k in range(zero):
            at = pl.ds(k * (src.shape[0] // zero), src.shape[0] // zero)
            copies.append((src.at[at], dst.at[at]))
    for k in range(zero):
        copies.append((down.at[:, k], out_down.at[:, :, k * rows : (k + 1) * rows]))
    copies += list(zip(small, small_out))
    copies = [pltpu.make_async_copy(s, d, sem.at[i]) for i, (s, d) in enumerate(copies)]
    for c in copies:
        c.start()
    for c in copies:
        c.wait()


def fast_device(sizes, mg, sg, mu, su, md, sd, router_weight, router_gain):
    bank, zero = sizes
    experts, rows, width = mg.shape
    piece = width // zero
    c = router_weight.shape[1]
    groups = 3 * experts // GROUP
    folds = zero.bit_length() - 2
    anywhere = pl.BlockSpec(memory_space=pl.ANY)
    vmem = pl.BlockSpec(memory_space=pltpu.VMEM)
    shapes = (
        ((experts, zero * rows, piece), bf16),
        ((experts, zero * rows, piece), bf16),
        ((experts, zero, piece, rows), bf16),
        ((experts, piece), f32),
        ((experts, piece), f32),
        ((experts, piece), f32),
        ((bank * c, zero * rows), bf16),
    )
    dma = pltpu.SemaphoreType.DMA
    landed = pl.pallas_call(
        functools.partial(exchange_kernel, bank, zero),
        in_specs=[anywhere] * 8,
        out_specs=[vmem] * 7,
        out_shape=[pltpu.VMEM(*s) for s in shapes],
        scratch_shapes=[
            pltpu.VMEM((AHEAD, rows, width), f32),
            pltpu.VMEM((AHEAD, rows, width), bf16),
            pltpu.VMEM((AHEAD, width, rows), f32),
            pltpu.VMEM((AHEAD, width, rows), bf16),
            pltpu.VMEM((READS, rows, width), f32),
            pltpu.VMEM((READS, rows, width), bf16),
            pltpu.VMEM((READS, width, rows), f32),
            pltpu.VMEM((READS, width, rows), bf16),
            pltpu.VMEM((SLOTS, zero - 1, rows, piece), bf16),
            pltpu.VMEM((SLOTS, zero - 1, piece, rows), bf16),
            pltpu.VMEM((FIRST, width), f32),
            pltpu.VMEM((zero - 1, FIRST, width), f32),
            pltpu.VMEM((zero, FIRST, piece), f32),
            pltpu.VMEM((groups, GROUP, width), f32),
            pltpu.VMEM((zero - 1, GROUP, piece), f32),
            pltpu.VMEM((groups, GROUP, width // 2), f32),
            pltpu.VMEM((groups, folds, GROUP, width // 2), f32),
            pltpu.VMEM((groups, folds, GROUP, width // 2), f32),
            pltpu.VMEM((groups, GROUP, width), f32),
            pltpu.VMEM((groups, zero, GROUP, piece), f32),
            pltpu.VMEM((c, rows), f32),
            pltpu.VMEM((1, rows), f32),
            pltpu.VMEM((c, rows), bf16),
            dma((2, 2, AHEAD)),
            dma((2, 2, READS)),
            dma((2, SLOTS)),
            dma((3, zero - 1)),
            dma((6,)),
            dma((2 * folds + 4, groups)),
            dma((6,)),
        ],
        compiler_params=pltpu.CompilerParams(
            collective_id=0, has_side_effects=True, vmem_limit_bytes=34 << 20),
    )(mg, sg, mu, su, md, sd, router_weight.T, router_gain.reshape(1, -1))
    outs = shapes[:2] + (((experts, piece, zero * rows), bf16),) + shapes[3:]
    *stored, router = pl.pallas_call(
        functools.partial(store_kernel, zero),
        in_specs=[vmem] * 7,
        out_specs=[anywhere] * 7,
        out_shape=[jax.ShapeDtypeStruct(*s) for s in outs],
        scratch_shapes=[dma((3 * zero + 4,))],
        compiler_params=pltpu.CompilerParams(vmem_limit_bytes=1 << 20),
    )(*landed)
    return (*stored, router.T)


def mine(scale, zero):
    width = scale.shape[1] // zero
    return lax.dynamic_slice_in_dim(scale, lax.axis_index("zero") * width, width, axis=1)


def general_device(sizes, mg, sg, mu, su, md, sd, router_weight, router_gain):
    zero = sizes[1]
    model = mg.shape[1] * zero
    merged = (mg + sg.astype(f32), mu + su.astype(f32), md + sd.astype(f32))
    totals = lax.psum(
        tuple(jnp.sum(jnp.abs(m), axis=a) for m, a in zip(merged, (1, 1, 2))), "zero"
    )
    scales = tuple(t / model for t in totals)
    finals = tuple(
        lax.all_to_all(
            (m / jnp.expand_dims(s, a)).astype(bf16),
            "zero", split_axis=3 - a, concat_axis=a, tiled=True,
        )
        for m, s, a in zip(merged, scales, (1, 1, 2))
    )
    part_router = (router_weight * router_gain[:, None]).astype(bf16)
    row_router = lax.all_gather(part_router, "zero", axis=0, tiled=True)
    serve_router = lax.all_gather(row_router, "bank", axis=1, tiled=True)
    return finals + tuple(mine(s, zero) for s in scales) + (serve_router,)


def fits(sizes, mg, router_weight):
    zero = sizes[1]
    experts, rows, width = mg.shape
    c = router_weight.shape[1]
    if zero < 4 or zero & (zero - 1) or experts != 2 * GROUP or experts % zero:
        return False
    if width % zero or (width // zero) % 128 or rows % 256 or c % 16:
        return False
    unit = rows * width
    held = 3 * experts * unit * 2 + 2 * (6 * (AHEAD + READS) + 2 * SLOTS) * unit
    return held <= 52 << 20


def solution(mesh):
    sizes = (mesh.shape["bank"], mesh.shape["zero"])

    def on_device(*args):
        fast = fits(sizes, args[0], args[6])
        return (fast_device if fast else general_device)(sizes, *args)

    return jax.shard_map(
        on_device,
        mesh=mesh,
        in_specs=(
            P("bank", "zero", None),
            P("bank", "zero", None),
            P("bank", "zero", None),
            P("bank", "zero", None),
            P("bank", None, "zero"),
            P("bank", None, "zero"),
            P("zero", "bank"),
            P("zero"),
        ),
        out_specs=(
            P("bank", None, "zero"),
            P("bank", None, "zero"),
            P("bank", "zero", None),
            P("bank", "zero"),
            P("bank", "zero"),
            P("bank", "zero"),
            P(),
        ),
        check_vma=False,
    )
```

```python
import functools

import jax
import jax.numpy as jnp
from jax import lax
from jax.experimental import pallas as pl
from jax.experimental.pallas import tpu as pltpu
from jax.sharding import PartitionSpec as P

f32, bf16 = jnp.float32, jnp.bfloat16
MESH = pl.DeviceIdType.MESH
GROUP = 8
FIRST = 2
AHEAD = 4
READS = 2
SLOTS = 4
LATE = 10
LAST = 1


def flip(index, bits, size):
    out, bit = 0, 1
    while bit < size:
        own = (index // bit) % 2
        out = out + bit * ((1 - own) if bits & bit else own)
        bit *= 2
    return out


def even(zero):
    return range(zero - 2, 0, -2)


def send_order(zero):
    return sorted(range(1, zero), key=lambda d: (d == 1, d & 1, -d))


def exchange_kernel(bank, zero, *refs):
    (mg, sg, mu, su, md, sd, rw, gain,
     land_gate, land_up, land_down, scale_gate, scale_up, scale_down, router, held,
     sum_m, sum_s, sum_dm, sum_ds, in_m, in_s, in_dm, in_ds, stage, stage_down,
     first, first_got, first_inv, part, part_got, pair_got, fold, fold_got, total, inverse,
     rw_v, gain_v, router_part,
     sum_sem, in_sem, stage_sem, data_sem, small_sem, fold_sem, late_sem, router_sem) = refs
    experts, rows, width = mg.shape
    piece = width // zero
    model = rows * zero
    per = experts // GROUP
    early = experts - held.shape[0]
    me = lax.axis_index("zero")
    my_bank = lax.axis_index("bank")
    masters, seconds = (mg, mu, md), (sg, su, sd)
    lands = (land_gate, land_up, land_down)
    scales = (scale_gate, scale_up, scale_down)
    order = send_order(zero)
    folds = fold_sem.shape[0] // 2 - 2
    half = width // 2
    my_half = pl.ds(pl.multiple_of((me % 2) * half, half), half)
    its_half = pl.ds(pl.multiple_of((1 - me % 2) * half, half), half)

    def peer(d):
        return flip(me, d, zero)

    def columns(k):
        return pl.ds(pl.multiple_of(k * piece, piece), piece)

    def send(src, dst, send_sem, recv_sem, d):
        pltpu.make_async_remote_copy(
            src_ref=src, dst_ref=dst, send_sem=send_sem, recv_sem=recv_sem,
            device_id={"zero": peer(d)}, device_id_type=MESH,
        ).start()

    def await_bytes(ref, sem):
        pltpu.make_async_copy(ref, ref, sem).wait()

    def reads(m, e, slot, bufs, sem):
        return (
            pltpu.make_async_copy(masters[m].at[e], bufs[0].at[slot], sem.at[0, slot]),
            pltpu.make_async_copy(seconds[m].at[e], bufs[1].at[slot], sem.at[1, slot]),
        )

    def sum_reads(m, e, slot):
        bufs = (sum_m, sum_s) if m < 2 else (sum_dm, sum_ds)
        return reads(m, e, slot, bufs, sum_sem.at[int(m == 2)])

    def scale_reads(m, e, slot):
        bufs = (in_m, in_s) if m < 2 else (in_dm, in_ds)
        return reads(m, e, slot, bufs, in_sem.at[int(m == 2)])

    def start(copies):
        for c in copies:
            c.start()

    def finish(copies):
        for c in copies:
            c.wait()


    def row_sum(m_ref, s_ref):
        def body(i, acc):
            r = pl.ds(pl.multiple_of(i * 16, 16), 16)
            x = jnp.abs(m_ref[r, :] + s_ref[r, :].astype(f32))
            return acc + (x[:8] + x[8:])

        acc = lax.fori_loop(0, rows // 16, body, jnp.zeros((8, width), f32), unroll=4)
        return jnp.sum(acc, axis=0, keepdims=True)

    def store_column_sums(m_ref, s_ref, g, j):
        found = []
        for k in range(width // 128):
            r = slice(k * 128, (k + 1) * 128)
            acc = None
            for c in range(rows // 128):
                cut = slice(c * 128, (c + 1) * 128)
                x = jnp.abs(m_ref[r, cut] + s_ref[r, cut].astype(f32))
                acc = x if acc is None else acc + x
            found.append(jnp.sum(acc.T, axis=0, keepdims=True))
        part[g, pl.ds(j, 1), :] = jnp.concatenate(found, axis=1)

    def sum_first():
        for j in range(FIRST):
            finish(scale_reads(0, j, j))
            v = row_sum(in_m.at[j], in_s.at[j])
            part[0, j : j + 1, :] = v
            first[j] = v
            if j == 0:
                pl.semaphore_wait(barrier, zero - 1 + bank - 1)
            for d in order:
                send(first.at[j], first_got.at[j, d - 1],
                     small_sem.at[4 + 2 * j], small_sem.at[5 + 2 * j], d)

    def sum_experts(g, low=0):
        m, base = g // per, (g % per) * GROUP

        def body(j, _):
            slot = lax.rem(j, AHEAD)
            finish(sum_reads(m, base + j, slot))
            if m < 2:
                v = row_sum(sum_m.at[slot], sum_s.at[slot])
                part[g, pl.ds(j, 1), :] = v
            else:
                store_column_sums(sum_dm.at[slot], sum_ds.at[slot], g, j)

            @pl.when(j + AHEAD < GROUP)
            def _():
                start(sum_reads(m, base + j + AHEAD, slot))

            return 0

        lax.fori_loop(low, GROUP, body, 0)
        if g + 1 < 3 * per:
            for j in range(AHEAD):
                start(sum_reads((g + 1) // per, ((g + 1) % per) * GROUP + j, j))

    def scatter_sums():
        for d in order:
            send(part.at[0, :, columns(peer(d))], part_got.at[d - 1],
                 small_sem.at[0], small_sem.at[1], d)

    def gather_totals():
        await_bytes(part_got, small_sem.at[1])
        t = part[0, :, columns(me)]
        for d in range(1, zero):
            t = t + part_got[d - 1]
        total[0, :, columns(me)] = t
        scales[0][:GROUP, :] = t / model
        for d in order:
            mine = total.at[0, :, columns(me)]
            send(mine, mine, small_sem.at[2], small_sem.at[3], d)

    def take_totals(g):
        if g:
            await_bytes(pair_got.at[g], fold_sem.at[2 * folds + 3, g])
            m, base = g // per, (g % per) * GROUP
            scales[m][base : base + GROUP, :] = total[g, :, columns(me)] / model
        else:
            await_bytes(part_got, small_sem.at[3])
        for k in range(zero):
            inverse[g, k] = 1.0 / (total[g, :, k * piece : (k + 1) * piece] / model)

    def pair_sums(g):
        send(part.at[g, :, its_half], pair_got.at[g], fold_sem.at[0, g], fold_sem.at[1, g], 1)

    def fold_sums(g, i):
        for i in range(i, folds + 1 if i == 2 else min(i, folds) + 1):
            if i:
                await_bytes(pair_got.at[g], fold_sem.at[2 * i + 1, g])
                h = fold[g, i - 1] + fold_got[g, i - 1]
            else:
                await_bytes(pair_got.at[g], fold_sem.at[1, g])
                h = part[g, :, my_half] + pair_got[g]
            sems = fold_sem.at[2 * i + 2, g], fold_sem.at[2 * i + 3, g]
            if i < folds:
                fold[g, i] = h
                send(fold.at[g, i], fold_got.at[g, i], *sems, 2 << i)
            else:
                total[g, :, my_half] = h
                there = total.at[g, :, my_half]
                send(there, there, *sems, 1)


    def send_expert(m, e, row, slot, before=0, hold=False, ready=False):
        if not ready:
            finish(scale_reads(m, e, lax.rem(e, READS)))
        b = lax.rem(e, READS)
        staged = stage if m < 2 else stage_down
        sem = stage_sem.at[int(m == 2), slot]
        if before:
            await_bytes(staged.at[slot, pl.ds(0, before)], sem)
        lot = rows // 2
        for d in order + [0]:
            k = peer(d)
            cut = columns(k)
            scale = row(k)
            if m < 2:
                for h in range(2):
                    r = slice(h * lot, (h + 1) * lot)
                    x = (in_m[b, r, cut] + in_s[b, r, cut].astype(f32)) * scale
                    if d:
                        stage[slot, d - 1, r, :] = x.astype(bf16)
                    else:
                        at = pl.ds(pl.multiple_of(me * rows + h * lot, lot), lot)
                        lands[m][e, at, :] = x.astype(bf16)
                there = lands[m].at[e, pl.ds(pl.multiple_of(me * rows, rows), rows)]
            else:
                t = jnp.broadcast_to(scale, (128, piece)).T
                for c in range(rows // 128):
                    r = slice(c * 128, (c + 1) * 128)
                    x = (in_dm[b, cut, r] + in_ds[b, cut, r].astype(f32)) * t
                    if d and hold and d % 2 == 0:
                        held[e - early, d // 2 - 1, :, r] = x.astype(bf16)
                    elif d:
                        stage_down[slot, d - 1, :, r] = x.astype(bf16)
                    else:
                        land_down[e, me, :, r] = x.astype(bf16)
                there = land_down.at[e, me]
            if d and not (hold and d % 2 == 0):
                send(staged.at[slot, d - 1], there, sem, data_sem.at[m, d - 1], d)

    def scaled_row(g, j):
        return lambda k: inverse[g, k, pl.ds(j, 1), :]

    def send_range(m, low, high, before=zero - 1, hold=False):
        def body(e, _):
            send_expert(m, e, scaled_row(m * per + e // GROUP, lax.rem(e, GROUP)),
                        lax.rem(e, SLOTS), before, hold)

            @pl.when(e + READS < experts)
            def _():
                start(scale_reads(m, e + READS, lax.rem(e, READS)))

            return 0

        lax.fori_loop(low, high, body, 0)


    c = rw.shape[0]
    own_experts = pl.ds(pl.multiple_of(my_bank * c, c), c)
    own_rows = pl.ds(pl.multiple_of(me * rows, rows), rows)

    def router_reads():
        return (
            pltpu.make_async_copy(rw, rw_v, router_sem.at[0]),
            pltpu.make_async_copy(gain, gain_v, router_sem.at[1]),
        )

    def fold_router():
        finish(router_reads())
        router_part[...] = (rw_v[...] * gain_v[...]).astype(bf16)
        router[own_experts, own_rows] = router_part[...]

    def send_router():
        for d in order:
            send(router_part, router.at[own_experts, own_rows], router_sem.at[2], router_sem.at[3], d)

    def share_router():
        await_bytes(router.at[pl.ds(0, c), pl.ds(0, (zero - 1) * rows)], router_sem.at[3])
        for d in range(1, bank):
            pltpu.make_async_remote_copy(
                src_ref=router.at[own_experts], dst_ref=router.at[own_experts],
                send_sem=router_sem.at[4], recv_sem=router_sem.at[5],
                device_id={"bank": (my_bank + d) % bank}, device_id_type=MESH,
            ).start()


    barrier = pltpu.get_barrier_semaphore()
    for d in range(1, zero):
        pl.semaphore_signal(barrier, inc=1, device_id={"zero": peer(d)}, device_id_type=MESH)
    for d in range(1, bank):
        pl.semaphore_signal(
            barrier, inc=1, device_id={"bank": (my_bank + d) % bank}, device_id_type=MESH)

    start(router_reads())
    for j in range(FIRST):
        start(scale_reads(0, j, j))
    fold_router()
    for j in range(FIRST, FIRST + AHEAD):
        start(sum_reads(0, j, j % AHEAD))
    sum_first()
    send_router()
    sum_experts(0, FIRST)
    scatter_sums()
    def send_first(j):
        await_bytes(first_got.at[j], small_sem.at[5 + 2 * j])
        t = first[j]
        for d in range(1, zero):
            t = t + first_got[j, d - 1]
        for k in range(zero):
            first_inv[j, k] = 1.0 / (t[:, k * piece : (k + 1) * piece] / model)
        send_expert(0, j, lambda k: first_inv[j, k], j, ready=True)
        start(scale_reads(0, j + READS, j % READS))

    send_first(0)
    sum_experts(1)
    pair_sums(1)
    gather_totals()
    send_first(1)
    fold_sums(1, 0)
    take_totals(0)
    send_range(0, 2, 4, before=0)
    sum_experts(2)
    pair_sums(2)
    fold_sums(1, 1)
    fold_sums(2, 0)
    send_range(0, 4, 6)
    fold_sums(1, 2)
    fold_sums(2, 1)
    sum_experts(3)
    pair_sums(3)
    send_range(0, 6, 7)
    fold_sums(3, 0)
    send_range(0, 7, 8)
    take_totals(1)
    send_range(0, 8, 10)
    fold_sums(2, 2)
    fold_sums(3, 1)
    sum_experts(4)
    pair_sums(4)
    send_range(0, 10, 11)
    fold_sums(4, 0)
    send_range(0, 11, 12)
    fold_sums(3, 2)
    fold_sums(4, 1)
    sum_experts(5)
    pair_sums(5)
    send_range(0, 12, 13)
    fold_sums(5, 0)
    share_router()
    send_range(0, 13, 14)
    fold_sums(4, 2)
    fold_sums(5, 1)
    send_range(0, 14, 16)
    for j in range(READS):
        start(scale_reads(1, j, j))
        start(scale_reads(2, j, j))
    fold_sums(5, 2)
    take_totals(2)
    take_totals(3)
    send_range(1, 0, 2)
    take_totals(4)
    take_totals(5)
    send_range(1, 2, experts)
    send_range(2, 0, SLOTS, before=0)
    send_range(2, SLOTS, early)
    send_range(2, early, early + SLOTS, hold=True)
    send_range(2, early + SLOTS, experts, before=zero // 2, hold=True)

    @pl.when(me % 2 != LAST)
    def _():
        def body(e, _):
            for d in even(zero):
                send(held.at[e, d // 2 - 1], land_down.at[early + e, me],
                     late_sem.at[0], late_sem.at[1], d)
            return 0

        lax.fori_loop(0, experts - early, body, 0)

    for s in range(SLOTS):
        await_bytes(stage.at[s], stage_sem.at[0, s])
        await_bytes(stage_down.at[s, pl.ds(0, zero // 2)], stage_sem.at[1, s])
    for j in range(FIRST):
        await_bytes(first_got.at[j], small_sem.at[4 + 2 * j])
    await_bytes(part_got, small_sem.at[0])
    await_bytes(part_got, small_sem.at[2])
    for g in range(1, 3 * per):
        for i in range(folds + 2):
            await_bytes(pair_got.at[g], fold_sem.at[2 * i, g])
    await_bytes(router.at[pl.ds(0, c), pl.ds(0, (zero - 1) * rows)], router_sem.at[2])
    if bank > 1:
        await_bytes(router.at[pl.ds(0, (bank - 1) * c)], router_sem.at[4])
        await_bytes(router.at[pl.ds(0, (bank - 1) * c)], router_sem.at[5])
    for d in range(1, zero):
        await_bytes(land_gate.at[:, pl.ds(0, rows)], data_sem.at[0, d - 1])
        await_bytes(land_up.at[:, pl.ds(0, rows)], data_sem.at[1, d - 1])
        await_bytes(land_down.at[pl.ds(0, experts if d % 2 else early), 0], data_sem.at[2, d - 1])

    @pl.when(me % 2 != LAST)
    def _():
        await_bytes(held, late_sem.at[0])
        await_bytes(held, late_sem.at[1])


def late_kernel(zero, held, stored, late, late_sem):
    me = lax.axis_index("zero")

    @pl.when(me % 2 == LAST)
    def _():
        barrier = pltpu.get_barrier_semaphore()
        for d in even(zero):
            pl.semaphore_signal(
                barrier, inc=1, device_id={"zero": flip(me, d, zero)}, device_id_type=MESH)
        pl.semaphore_wait(barrier, zero // 2 - 1)

        def body(e, _):
            for d in even(zero):
                pltpu.make_async_remote_copy(
                    src_ref=held.at[e, d // 2 - 1], dst_ref=late.at[e, d // 2 - 1],
                    send_sem=late_sem.at[0], recv_sem=late_sem.at[1],
                    device_id={"zero": flip(me, d, zero)}, device_id_type=MESH,
                ).start()
            return 0

        lax.fori_loop(0, held.shape[0], body, 0)
        for i in range(2):
            pltpu.make_async_copy(held, held, late_sem.at[i]).wait()


def place_kernel(zero, down, late, out, sem):
    me = lax.axis_index("zero")
    count, _, piece, rows = late.shape
    experts = out.shape[0]

    @pl.when(me % 2 == LAST)
    def _():
        copies = []
        for d in even(zero):
            at = pl.ds(pl.multiple_of(flip(me, d, zero) * rows, rows), rows)
            copies.append(pltpu.make_async_copy(
                late.at[:, d // 2 - 1], out.at[pl.ds(experts - count, count), :, at],
                sem.at[d // 2 - 1]))
        for c in copies:
            c.start()
        for c in copies:
            c.wait()


def store_kernel(zero, *refs):
    gate, up, down, *small = refs[:7]
    out_gate, out_up, out_down, *small_out = refs[7:14]
    token, sem = refs[14:]
    token[...] = jnp.zeros_like(token)
    rows = down.shape[3]
    copies = []
    for src, dst in ((gate, out_gate), (up, out_up)):
        for k in range(zero):
            at = pl.ds(k * (src.shape[0] // zero), src.shape[0] // zero)
            copies.append((src.at[at], dst.at[at]))
    for k in range(zero):
        copies.append((down.at[:, k], out_down.at[:, :, k * rows : (k + 1) * rows]))
    copies += list(zip(small, small_out))
    copies = [pltpu.make_async_copy(s, d, sem.at[i]) for i, (s, d) in enumerate(copies)]
    for c in copies:
        c.start()
    for c in copies:
        c.wait()


def fast_device(sizes, mg, sg, mu, su, md, sd, router_weight, router_gain):
    bank, zero = sizes
    experts, rows, width = mg.shape
    piece = width // zero
    c = router_weight.shape[1]
    groups = 3 * experts // GROUP
    folds = zero.bit_length() - 2
    anywhere = pl.BlockSpec(memory_space=pl.ANY)
    vmem = pl.BlockSpec(memory_space=pltpu.VMEM)
    shapes = (
        ((experts, zero * rows, piece), bf16),
        ((experts, zero * rows, piece), bf16),
        ((experts, zero, piece, rows), bf16),
        ((experts, piece), f32),
        ((experts, piece), f32),
        ((experts, piece), f32),
        ((bank * c, zero * rows), bf16),
        ((experts * LATE // 16, zero // 2 - 1, piece, rows), bf16),
    )
    dma = pltpu.SemaphoreType.DMA
    *landed, held = pl.pallas_call(
        functools.partial(exchange_kernel, bank, zero),
        in_specs=[anywhere] * 8,
        out_specs=[vmem] * 8,
        out_shape=[pltpu.VMEM(*s) for s in shapes],
        scratch_shapes=[
            pltpu.VMEM((AHEAD, rows, width), f32),
            pltpu.VMEM((AHEAD, rows, width), bf16),
            pltpu.VMEM((AHEAD, width, rows), f32),
            pltpu.VMEM((AHEAD, width, rows), bf16),
            pltpu.VMEM((READS, rows, width), f32),
            pltpu.VMEM((READS, rows, width), bf16),
            pltpu.VMEM((READS, width, rows), f32),
            pltpu.VMEM((READS, width, rows), bf16),
            pltpu.VMEM((SLOTS, zero - 1, rows, piece), bf16),
            pltpu.VMEM((SLOTS, zero - 1, piece, rows), bf16),
            pltpu.VMEM((FIRST, 1, width), f32),
            pltpu.VMEM((FIRST, zero - 1, 1, width), f32),
            pltpu.VMEM((FIRST, zero, 1, piece), f32),
            pltpu.VMEM((groups, GROUP, width), f32),
            pltpu.VMEM((zero - 1, GROUP, piece), f32),
            pltpu.VMEM((groups, GROUP, width // 2), f32),
            pltpu.VMEM((groups, folds, GROUP, width // 2), f32),
            pltpu.VMEM((groups, folds, GROUP, width // 2), f32),
            pltpu.VMEM((groups, GROUP, width), f32),
            pltpu.VMEM((groups, zero, GROUP, piece), f32),
            pltpu.VMEM((c, rows), f32),
            pltpu.VMEM((1, rows), f32),
            pltpu.VMEM((c, rows), bf16),
            dma((2, 2, AHEAD)),
            dma((2, 2, READS)),
            dma((2, SLOTS)),
            dma((3, zero - 1)),
            dma((4 + 2 * FIRST,)),
            dma((2 * folds + 4, groups)),
            dma((2,)),
            dma((6,)),
        ],
        compiler_params=pltpu.CompilerParams(
            collective_id=0, has_side_effects=True, vmem_limit_bytes=34 << 20),
    )(mg, sg, mu, su, md, sd, router_weight.T, router_gain.reshape(1, -1))
    token = ((8, 128), f32)
    outs = shapes[:2] + (((experts, piece, zero * rows), bf16),) + shapes[3:7]
    *stored, router, token = pl.pallas_call(
        functools.partial(store_kernel, zero),
        in_specs=[vmem] * 7,
        out_specs=[anywhere] * 7 + [vmem],
        out_shape=[jax.ShapeDtypeStruct(*s) for s in outs] + [pltpu.VMEM(*token)],
        scratch_shapes=[dma((3 * zero + 4,))],
        compiler_params=pltpu.CompilerParams(vmem_limit_bytes=1 << 20),
    )(*landed)
    gate, up, down, *scales = stored
    late = pl.pallas_call(
        functools.partial(late_kernel, zero),
        in_specs=[vmem, vmem],
        out_specs=vmem,
        out_shape=pltpu.VMEM(*shapes[7]),
        scratch_shapes=[dma((2,))],
        compiler_params=pltpu.CompilerParams(
            collective_id=1, has_side_effects=True, vmem_limit_bytes=1 << 20),
    )(held, token)
    down = pl.pallas_call(
        functools.partial(place_kernel, zero),
        in_specs=[anywhere, vmem],
        out_specs=anywhere,
        out_shape=jax.ShapeDtypeStruct(*outs[2]),
        input_output_aliases={0: 0},
        scratch_shapes=[dma((zero // 2 - 1,))],
        compiler_params=pltpu.CompilerParams(vmem_limit_bytes=1 << 20),
    )(down, late)
    return (gate, up, down, *scales, router.T)


def mine(scale, zero):
    width = scale.shape[1] // zero
    return lax.dynamic_slice_in_dim(scale, lax.axis_index("zero") * width, width, axis=1)


def general_device(sizes, mg, sg, mu, su, md, sd, router_weight, router_gain):
    zero = sizes[1]
    model = mg.shape[1] * zero
    merged = (mg + sg.astype(f32), mu + su.astype(f32), md + sd.astype(f32))
    totals = lax.psum(
        tuple(jnp.sum(jnp.abs(m), axis=a) for m, a in zip(merged, (1, 1, 2))), "zero"
    )
    scales = tuple(t / model for t in totals)
    finals = tuple(
        lax.all_to_all(
            (m / jnp.expand_dims(s, a)).astype(bf16),
            "zero", split_axis=3 - a, concat_axis=a, tiled=True,
        )
        for m, s, a in zip(merged, scales, (1, 1, 2))
    )
    part_router = (router_weight * router_gain[:, None]).astype(bf16)
    row_router = lax.all_gather(part_router, "zero", axis=0, tiled=True)
    serve_router = lax.all_gather(row_router, "bank", axis=1, tiled=True)
    return finals + tuple(mine(s, zero) for s in scales) + (serve_router,)


def fits(sizes, mg, router_weight):
    zero = sizes[1]
    experts, rows, width = mg.shape
    c = router_weight.shape[1]
    if zero < 4 or zero & (zero - 1) or experts != 2 * GROUP or experts % zero:
        return False
    if width % zero or (width // zero) % 128 or rows % 256 or c % 16:
        return False
    unit = rows * width
    held = 3 * experts * unit * 2 + 2 * (6 * (AHEAD + READS) + 2 * SLOTS) * unit
    return held <= 52 << 20


def solution(mesh):
    sizes = (mesh.shape["bank"], mesh.shape["zero"])

    def on_device(*args):
        fast = fits(sizes, args[0], args[6])
        return (fast_device if fast else general_device)(sizes, *args)

    return jax.shard_map(
        on_device,
        mesh=mesh,
        in_specs=(
            P("bank", "zero", None),
            P("bank", "zero", None),
            P("bank", "zero", None),
            P("bank", "zero", None),
            P("bank", None, "zero"),
            P("bank", None, "zero"),
            P("zero", "bank"),
            P("zero"),
        ),
        out_specs=(
            P("bank", None, "zero"),
            P("bank", None, "zero"),
            P("bank", "zero", None),
            P("bank", "zero"),
            P("bank", "zero"),
            P("bank", "zero"),
            P(),
        ),
        check_vma=False,
    )
```

```python
import functools

import jax
import jax.numpy as jnp
from jax import lax
from jax.experimental import pallas as pl
from jax.experimental.pallas import tpu as pltpu
from jax.sharding import PartitionSpec as P

f32, bf16 = jnp.float32, jnp.bfloat16
MESH = pl.DeviceIdType.MESH
GROUP = 8
FIRST = 2
AHEAD = 4
READS = 2
SLOTS = 4
LATE = 10
LAST = 1


def flip(index, bits, size):
    out, bit = 0, 1
    while bit < size:
        own = (index // bit) % 2
        out = out + bit * ((1 - own) if bits & bit else own)
        bit *= 2
    return out


def even(zero):
    return range(zero - 2, 0, -2)


def send_order(zero):
    return sorted(range(1, zero), key=lambda d: (d == 1, d & 1, -d))


def exchange_kernel(bank, zero, *refs):
    (mg, sg, mu, su, md, sd, rw, gain,
     land_gate, land_up, land_down, scale_gate, scale_up, scale_down, router, held,
     sum_m, sum_s, sum_dm, sum_ds, in_m, in_s, in_dm, in_ds, stage, stage_down,
     first, first_got, first_inv, part, part_got, pair_got, fold, fold_got, total, inverse,
     rw_v, gain_v, router_part,
     sum_sem, in_sem, stage_sem, data_sem, small_sem, fold_sem, late_sem, router_sem) = refs
    experts, rows, width = mg.shape
    piece = width // zero
    model = rows * zero
    per = experts // GROUP
    early = experts - held.shape[0]
    me = lax.axis_index("zero")
    my_bank = lax.axis_index("bank")
    masters, seconds = (mg, mu, md), (sg, su, sd)
    lands = (land_gate, land_up, land_down)
    scales = (scale_gate, scale_up, scale_down)
    order = send_order(zero)
    folds = fold_sem.shape[0] // 2 - 2
    half = width // 2
    my_half = pl.ds(pl.multiple_of((me % 2) * half, half), half)
    its_half = pl.ds(pl.multiple_of((1 - me % 2) * half, half), half)

    def peer(d):
        return flip(me, d, zero)

    def columns(k):
        return pl.ds(pl.multiple_of(k * piece, piece), piece)

    def send(src, dst, send_sem, recv_sem, d):
        pltpu.make_async_remote_copy(
            src_ref=src, dst_ref=dst, send_sem=send_sem, recv_sem=recv_sem,
            device_id={"zero": peer(d)}, device_id_type=MESH,
        ).start()

    def await_bytes(ref, sem):
        pltpu.make_async_copy(ref, ref, sem).wait()

    def reads(m, e, slot, bufs, sem):
        return (
            pltpu.make_async_copy(masters[m].at[e], bufs[0].at[slot], sem.at[0, slot]),
            pltpu.make_async_copy(seconds[m].at[e], bufs[1].at[slot], sem.at[1, slot]),
        )

    def sum_reads(m, e, slot):
        bufs = (sum_m, sum_s) if m < 2 else (sum_dm, sum_ds)
        return reads(m, e, slot, bufs, sum_sem.at[int(m == 2)])

    def scale_reads(m, e, slot):
        bufs = (in_m, in_s) if m < 2 else (in_dm, in_ds)
        return reads(m, e, slot, bufs, in_sem.at[int(m == 2)])

    def start(copies):
        for c in copies:
            c.start()

    def finish(copies):
        for c in copies:
            c.wait()


    def row_sum(m_ref, s_ref):
        def body(i, acc):
            r = pl.ds(pl.multiple_of(i * 16, 16), 16)
            x = jnp.abs(m_ref[r, :] + s_ref[r, :].astype(f32))
            return acc + (x[:8] + x[8:])

        acc = lax.fori_loop(0, rows // 16, body, jnp.zeros((8, width), f32), unroll=4)
        return jnp.sum(acc, axis=0, keepdims=True)

    def store_column_sums(m_ref, s_ref, g, j):
        found = []
        for k in range(width // 128):
            r = slice(k * 128, (k + 1) * 128)
            acc = None
            for c in range(rows // 128):
                cut = slice(c * 128, (c + 1) * 128)
                x = jnp.abs(m_ref[r, cut] + s_ref[r, cut].astype(f32))
                acc = x if acc is None else acc + x
            found.append(jnp.sum(acc.T, axis=0, keepdims=True))
        part[g, pl.ds(j, 1), :] = jnp.concatenate(found, axis=1)

    def sum_first():
        for j in range(FIRST):
            finish(scale_reads(0, j, j))
            if j == 0:
                for i in range(FIRST, FIRST + AHEAD):
                    start(sum_reads(0, i, i % AHEAD))
            v = row_sum(in_m.at[j], in_s.at[j])
            part[0, j : j + 1, :] = v
            first[j] = v
            if j == 0:
                pl.semaphore_wait(barrier, zero - 1 + bank - 1)
            for d in order:
                send(first.at[j], first_got.at[j, d - 1],
                     small_sem.at[4 + 2 * j], small_sem.at[5 + 2 * j], d)

    def sum_experts(g, low=0):
        m, base = g // per, (g % per) * GROUP

        def body(j, _):
            slot = lax.rem(j, AHEAD)
            finish(sum_reads(m, base + j, slot))
            if m < 2:
                v = row_sum(sum_m.at[slot], sum_s.at[slot])
                part[g, pl.ds(j, 1), :] = v
            else:
                store_column_sums(sum_dm.at[slot], sum_ds.at[slot], g, j)

            @pl.when(j + AHEAD < GROUP)
            def _():
                start(sum_reads(m, base + j + AHEAD, slot))

            return 0

        lax.fori_loop(low, GROUP, body, 0)
        if g + 1 < 3 * per:
            for j in range(AHEAD):
                start(sum_reads((g + 1) // per, ((g + 1) % per) * GROUP + j, j))

    def scatter_sums():
        for d in order:
            send(part.at[0, :, columns(peer(d))], part_got.at[d - 1],
                 small_sem.at[0], small_sem.at[1], d)

    def gather_totals():
        await_bytes(part_got, small_sem.at[1])
        t = part[0, :, columns(me)]
        for d in range(1, zero):
            t = t + part_got[d - 1]
        total[0, :, columns(me)] = t
        scales[0][:GROUP, :] = t / model
        for d in order:
            mine = total.at[0, :, columns(me)]
            send(mine, mine, small_sem.at[2], small_sem.at[3], d)

    def take_totals(g):
        if g:
            await_bytes(pair_got.at[g], fold_sem.at[2 * folds + 3, g])
            m, base = g // per, (g % per) * GROUP
            scales[m][base : base + GROUP, :] = total[g, :, columns(me)] / model
        else:
            await_bytes(part_got, small_sem.at[3])
        for k in range(zero):
            inverse[g, k] = 1.0 / (total[g, :, k * piece : (k + 1) * piece] / model)

    def pair_sums(g):
        send(part.at[g, :, its_half], pair_got.at[g], fold_sem.at[0, g], fold_sem.at[1, g], 1)

    def fold_sums(g, i):
        for i in range(i, folds + 1 if i == 2 else min(i, folds) + 1):
            if i:
                await_bytes(pair_got.at[g], fold_sem.at[2 * i + 1, g])
                h = fold[g, i - 1] + fold_got[g, i - 1]
            else:
                await_bytes(pair_got.at[g], fold_sem.at[1, g])
                h = part[g, :, my_half] + pair_got[g]
            sems = fold_sem.at[2 * i + 2, g], fold_sem.at[2 * i + 3, g]
            if i < folds:
                fold[g, i] = h
                send(fold.at[g, i], fold_got.at[g, i], *sems, 2 << i)
            else:
                total[g, :, my_half] = h
                there = total.at[g, :, my_half]
                send(there, there, *sems, 1)


    def send_expert(m, e, row, slot, before=0, hold=False, ready=False):
        if not ready:
            finish(scale_reads(m, e, lax.rem(e, READS)))
        b = lax.rem(e, READS)
        staged = stage if m < 2 else stage_down
        sem = stage_sem.at[int(m == 2), slot]
        if before:
            await_bytes(staged.at[slot, pl.ds(0, before)], sem)
        lot = rows // 2
        for d in order + [0]:
            k = peer(d)
            cut = columns(k)
            scale = row(k)
            if m < 2:
                for h in range(2):
                    r = slice(h * lot, (h + 1) * lot)
                    x = (in_m[b, r, cut] + in_s[b, r, cut].astype(f32)) * scale
                    if d:
                        stage[slot, d - 1, r, :] = x.astype(bf16)
                    else:
                        at = pl.ds(pl.multiple_of(me * rows + h * lot, lot), lot)
                        lands[m][e, at, :] = x.astype(bf16)
                there = lands[m].at[e, pl.ds(pl.multiple_of(me * rows, rows), rows)]
            else:
                t = jnp.broadcast_to(scale, (128, piece)).T
                for c in range(rows // 128):
                    r = slice(c * 128, (c + 1) * 128)
                    x = (in_dm[b, cut, r] + in_ds[b, cut, r].astype(f32)) * t
                    if d and hold and d % 2 == 0:
                        held[e - early, d // 2 - 1, :, r] = x.astype(bf16)
                    elif d:
                        stage_down[slot, d - 1, :, r] = x.astype(bf16)
                    else:
                        land_down[e, me, :, r] = x.astype(bf16)
                there = land_down.at[e, me]
            if d and not (hold and d % 2 == 0):
                send(staged.at[slot, d - 1], there, sem, data_sem.at[m, d - 1], d)

    def scaled_row(g, j):
        return lambda k: inverse[g, k, pl.ds(j, 1), :]

    def send_range(m, low, high, before=zero - 1, hold=False):
        def body(e, _):
            send_expert(m, e, scaled_row(m * per + e // GROUP, lax.rem(e, GROUP)),
                        lax.rem(e, SLOTS), before, hold)

            @pl.when(e + READS < experts)
            def _():
                start(scale_reads(m, e + READS, lax.rem(e, READS)))

            return 0

        lax.fori_loop(low, high, body, 0)


    c = rw.shape[0]
    own_experts = pl.ds(pl.multiple_of(my_bank * c, c), c)
    own_rows = pl.ds(pl.multiple_of(me * rows, rows), rows)

    def router_reads():
        return (
            pltpu.make_async_copy(rw, rw_v, router_sem.at[0]),
            pltpu.make_async_copy(gain, gain_v, router_sem.at[1]),
        )

    def fold_router():
        finish(router_reads())
        router_part[...] = (rw_v[...] * gain_v[...]).astype(bf16)
        router[own_experts, own_rows] = router_part[...]

    def send_router():
        for d in order:
            send(router_part, router.at[own_experts, own_rows], router_sem.at[2], router_sem.at[3], d)

    def share_router():
        await_bytes(router.at[pl.ds(0, c), pl.ds(0, (zero - 1) * rows)], router_sem.at[3])
        for d in range(1, bank):
            pltpu.make_async_remote_copy(
                src_ref=router.at[own_experts], dst_ref=router.at[own_experts],
                send_sem=router_sem.at[4], recv_sem=router_sem.at[5],
                device_id={"bank": (my_bank + d) % bank}, device_id_type=MESH,
            ).start()


    barrier = pltpu.get_barrier_semaphore()
    for d in range(1, zero):
        pl.semaphore_signal(barrier, inc=1, device_id={"zero": peer(d)}, device_id_type=MESH)
    for d in range(1, bank):
        pl.semaphore_signal(
            barrier, inc=1, device_id={"bank": (my_bank + d) % bank}, device_id_type=MESH)

    start(router_reads())
    for j in range(FIRST):
        start(scale_reads(0, j, j))
    fold_router()
    sum_first()
    send_router()
    sum_experts(0, FIRST)
    scatter_sums()
    def send_first(j):
        await_bytes(first_got.at[j], small_sem.at[5 + 2 * j])
        t = first[j]
        for d in range(1, zero):
            t = t + first_got[j, d - 1]
        for k in range(zero):
            first_inv[j, k] = 1.0 / (t[:, k * piece : (k + 1) * piece] / model)
        send_expert(0, j, lambda k: first_inv[j, k], j, ready=True)
        start(scale_reads(0, j + READS, j % READS))

    send_first(0)
    sum_experts(1)
    pair_sums(1)
    gather_totals()
    send_first(1)
    fold_sums(1, 0)
    take_totals(0)
    send_range(0, 2, 4, before=0)
    sum_experts(2)
    pair_sums(2)
    fold_sums(1, 1)
    fold_sums(2, 0)
    send_range(0, 4, 6)
    fold_sums(1, 2)
    fold_sums(2, 1)
    sum_experts(3)
    pair_sums(3)
    send_range(0, 6, 7)
    fold_sums(3, 0)
    send_range(0, 7, 8)
    take_totals(1)
    send_range(0, 8, 10)
    fold_sums(2, 2)
    fold_sums(3, 1)
    sum_experts(4)
    pair_sums(4)
    send_range(0, 10, 11)
    fold_sums(4, 0)
    send_range(0, 11, 13)
    sum_experts(5)
    pair_sums(5)
    fold_sums(3, 2)
    fold_sums(4, 1)
    send_range(0, 13, 14)
    fold_sums(5, 0)
    share_router()
    send_range(0, 14, 16)
    for j in range(READS):
        start(scale_reads(1, j, j))
        start(scale_reads(2, j, j))
    fold_sums(4, 2)
    fold_sums(5, 1)
    take_totals(2)
    take_totals(3)
    send_range(1, 0, 2)
    fold_sums(5, 2)
    send_range(1, 2, 4)
    take_totals(4)
    take_totals(5)
    send_range(1, 4, experts)
    send_range(2, 0, SLOTS, before=0)
    send_range(2, SLOTS, early)
    send_range(2, early, early + SLOTS, hold=True)
    send_range(2, early + SLOTS, experts, before=zero // 2, hold=True)

    @pl.when(me % 2 != LAST)
    def _():
        def body(e, _):
            for d in even(zero):
                send(held.at[e, d // 2 - 1], land_down.at[early + e, me],
                     late_sem.at[0], late_sem.at[1], d)
            return 0

        lax.fori_loop(0, experts - early, body, 0)

    for s in range(SLOTS):
        await_bytes(stage.at[s], stage_sem.at[0, s])
        await_bytes(stage_down.at[s, pl.ds(0, zero // 2)], stage_sem.at[1, s])
    for j in range(FIRST):
        await_bytes(first_got.at[j], small_sem.at[4 + 2 * j])
    await_bytes(part_got, small_sem.at[0])
    await_bytes(part_got, small_sem.at[2])
    for g in range(1, 3 * per):
        for i in range(folds + 2):
            await_bytes(pair_got.at[g], fold_sem.at[2 * i, g])
    await_bytes(router.at[pl.ds(0, c), pl.ds(0, (zero - 1) * rows)], router_sem.at[2])
    if bank > 1:
        await_bytes(router.at[pl.ds(0, (bank - 1) * c)], router_sem.at[4])
        await_bytes(router.at[pl.ds(0, (bank - 1) * c)], router_sem.at[5])
    for d in range(1, zero):
        await_bytes(land_gate.at[:, pl.ds(0, rows)], data_sem.at[0, d - 1])
        await_bytes(land_up.at[:, pl.ds(0, rows)], data_sem.at[1, d - 1])
        await_bytes(land_down.at[pl.ds(0, experts if d % 2 else early), 0], data_sem.at[2, d - 1])

    @pl.when(me % 2 != LAST)
    def _():
        await_bytes(held, late_sem.at[0])
        await_bytes(held, late_sem.at[1])


def late_kernel(zero, held, stored, late, late_sem):
    me = lax.axis_index("zero")

    @pl.when(me % 2 == LAST)
    def _():
        barrier = pltpu.get_barrier_semaphore()
        for d in even(zero):
            pl.semaphore_signal(
                barrier, inc=1, device_id={"zero": flip(me, d, zero)}, device_id_type=MESH)
        pl.semaphore_wait(barrier, zero // 2 - 1)

        def body(e, _):
            for d in even(zero):
                pltpu.make_async_remote_copy(
                    src_ref=held.at[e, d // 2 - 1], dst_ref=late.at[e, d // 2 - 1],
                    send_sem=late_sem.at[0], recv_sem=late_sem.at[1],
                    device_id={"zero": flip(me, d, zero)}, device_id_type=MESH,
                ).start()
            return 0

        lax.fori_loop(0, held.shape[0], body, 0)
        for i in range(2):
            pltpu.make_async_copy(held, held, late_sem.at[i]).wait()


def place_kernel(zero, down, late, out, sem):
    me = lax.axis_index("zero")
    count, _, piece, rows = late.shape
    experts = out.shape[0]

    @pl.when(me % 2 == LAST)
    def _():
        copies = []
        for d in even(zero):
            at = pl.ds(pl.multiple_of(flip(me, d, zero) * rows, rows), rows)
            copies.append(pltpu.make_async_copy(
                late.at[:, d // 2 - 1], out.at[pl.ds(experts - count, count), :, at],
                sem.at[d // 2 - 1]))
        for c in copies:
            c.start()
        for c in copies:
            c.wait()


def store_kernel(zero, *refs):
    gate, up, down, *small = refs[:7]
    out_gate, out_up, out_down, *small_out = refs[7:14]
    token, sem = refs[14:]
    token[...] = jnp.zeros_like(token)
    rows = down.shape[3]
    copies = []
    for src, dst in ((gate, out_gate), (up, out_up)):
        for k in range(zero):
            at = pl.ds(k * (src.shape[0] // zero), src.shape[0] // zero)
            copies.append((src.at[at], dst.at[at]))
    for k in range(zero):
        copies.append((down.at[:, k], out_down.at[:, :, k * rows : (k + 1) * rows]))
    copies += list(zip(small, small_out))
    copies = [pltpu.make_async_copy(s, d, sem.at[i]) for i, (s, d) in enumerate(copies)]
    for c in copies:
        c.start()
    for c in copies:
        c.wait()


def fast_device(sizes, mg, sg, mu, su, md, sd, router_weight, router_gain):
    bank, zero = sizes
    experts, rows, width = mg.shape
    piece = width // zero
    c = router_weight.shape[1]
    groups = 3 * experts // GROUP
    folds = zero.bit_length() - 2
    anywhere = pl.BlockSpec(memory_space=pl.ANY)
    vmem = pl.BlockSpec(memory_space=pltpu.VMEM)
    shapes = (
        ((experts, zero * rows, piece), bf16),
        ((experts, zero * rows, piece), bf16),
        ((experts, zero, piece, rows), bf16),
        ((experts, piece), f32),
        ((experts, piece), f32),
        ((experts, piece), f32),
        ((bank * c, zero * rows), bf16),
        ((experts * LATE // 16, zero // 2 - 1, piece, rows), bf16),
    )
    dma = pltpu.SemaphoreType.DMA
    *landed, held = pl.pallas_call(
        functools.partial(exchange_kernel, bank, zero),
        in_specs=[anywhere] * 8,
        out_specs=[vmem] * 8,
        out_shape=[pltpu.VMEM(*s) for s in shapes],
        scratch_shapes=[
            pltpu.VMEM((AHEAD, rows, width), f32),
            pltpu.VMEM((AHEAD, rows, width), bf16),
            pltpu.VMEM((AHEAD, width, rows), f32),
            pltpu.VMEM((AHEAD, width, rows), bf16),
            pltpu.VMEM((READS, rows, width), f32),
            pltpu.VMEM((READS, rows, width), bf16),
            pltpu.VMEM((READS, width, rows), f32),
            pltpu.VMEM((READS, width, rows), bf16),
            pltpu.VMEM((SLOTS, zero - 1, rows, piece), bf16),
            pltpu.VMEM((SLOTS, zero - 1, piece, rows), bf16),
            pltpu.VMEM((FIRST, 1, width), f32),
            pltpu.VMEM((FIRST, zero - 1, 1, width), f32),
            pltpu.VMEM((FIRST, zero, 1, piece), f32),
            pltpu.VMEM((groups, GROUP, width), f32),
            pltpu.VMEM((zero - 1, GROUP, piece), f32),
            pltpu.VMEM((groups, GROUP, width // 2), f32),
            pltpu.VMEM((groups, folds, GROUP, width // 2), f32),
            pltpu.VMEM((groups, folds, GROUP, width // 2), f32),
            pltpu.VMEM((groups, GROUP, width), f32),
            pltpu.VMEM((groups, zero, GROUP, piece), f32),
            pltpu.VMEM((c, rows), f32),
            pltpu.VMEM((1, rows), f32),
            pltpu.VMEM((c, rows), bf16),
            dma((2, 2, AHEAD)),
            dma((2, 2, READS)),
            dma((2, SLOTS)),
            dma((3, zero - 1)),
            dma((4 + 2 * FIRST,)),
            dma((2 * folds + 4, groups)),
            dma((2,)),
            dma((6,)),
        ],
        compiler_params=pltpu.CompilerParams(
            collective_id=0, has_side_effects=True, vmem_limit_bytes=34 << 20),
    )(mg, sg, mu, su, md, sd, router_weight.T, router_gain.reshape(1, -1))
    token = ((8, 128), f32)
    outs = shapes[:2] + (((experts, piece, zero * rows), bf16),) + shapes[3:7]
    *stored, router, token = pl.pallas_call(
        functools.partial(store_kernel, zero),
        in_specs=[vmem] * 7,
        out_specs=[anywhere] * 7 + [vmem],
        out_shape=[jax.ShapeDtypeStruct(*s) for s in outs] + [pltpu.VMEM(*token)],
        scratch_shapes=[dma((3 * zero + 4,))],
        compiler_params=pltpu.CompilerParams(vmem_limit_bytes=1 << 20),
    )(*landed)
    gate, up, down, *scales = stored
    late = pl.pallas_call(
        functools.partial(late_kernel, zero),
        in_specs=[vmem, vmem],
        out_specs=vmem,
        out_shape=pltpu.VMEM(*shapes[7]),
        scratch_shapes=[dma((2,))],
        compiler_params=pltpu.CompilerParams(
            collective_id=1, has_side_effects=True, vmem_limit_bytes=1 << 20),
    )(held, token)
    down = pl.pallas_call(
        functools.partial(place_kernel, zero),
        in_specs=[anywhere, vmem],
        out_specs=anywhere,
        out_shape=jax.ShapeDtypeStruct(*outs[2]),
        input_output_aliases={0: 0},
        scratch_shapes=[dma((zero // 2 - 1,))],
        compiler_params=pltpu.CompilerParams(vmem_limit_bytes=1 << 20),
    )(down, late)
    return (gate, up, down, *scales, router.T)


def mine(scale, zero):
    width = scale.shape[1] // zero
    return lax.dynamic_slice_in_dim(scale, lax.axis_index("zero") * width, width, axis=1)


def general_device(sizes, mg, sg, mu, su, md, sd, router_weight, router_gain):
    zero = sizes[1]
    model = mg.shape[1] * zero
    merged = (mg + sg.astype(f32), mu + su.astype(f32), md + sd.astype(f32))
    totals = lax.psum(
        tuple(jnp.sum(jnp.abs(m), axis=a) for m, a in zip(merged, (1, 1, 2))), "zero"
    )
    scales = tuple(t / model for t in totals)
    finals = tuple(
        lax.all_to_all(
            (m / jnp.expand_dims(s, a)).astype(bf16),
            "zero", split_axis=3 - a, concat_axis=a, tiled=True,
        )
        for m, s, a in zip(merged, scales, (1, 1, 2))
    )
    part_router = (router_weight * router_gain[:, None]).astype(bf16)
    row_router = lax.all_gather(part_router, "zero", axis=0, tiled=True)
    serve_router = lax.all_gather(row_router, "bank", axis=1, tiled=True)
    return finals + tuple(mine(s, zero) for s in scales) + (serve_router,)


def fits(sizes, mg, router_weight):
    zero = sizes[1]
    experts, rows, width = mg.shape
    c = router_weight.shape[1]
    if zero < 4 or zero & (zero - 1) or experts != 2 * GROUP or experts % zero:
        return False
    if width % zero or (width // zero) % 128 or rows % 256 or c % 16:
        return False
    unit = rows * width
    held = 3 * experts * unit * 2 + 2 * (6 * (AHEAD + READS) + 2 * SLOTS) * unit
    return held <= 52 << 20


def solution(mesh):
    sizes = (mesh.shape["bank"], mesh.shape["zero"])

    def on_device(*args):
        fast = fits(sizes, args[0], args[6])
        return (fast_device if fast else general_device)(sizes, *args)

    return jax.shard_map(
        on_device,
        mesh=mesh,
        in_specs=(
            P("bank", "zero", None),
            P("bank", "zero", None),
            P("bank", "zero", None),
            P("bank", "zero", None),
            P("bank", None, "zero"),
            P("bank", None, "zero"),
            P("zero", "bank"),
            P("zero"),
        ),
        out_specs=(
            P("bank", None, "zero"),
            P("bank", None, "zero"),
            P("bank", "zero", None),
            P("bank", "zero"),
            P("bank", "zero"),
            P("bank", "zero"),
            P(),
        ),
        check_vma=False,
    )
```
